32 devices in a mesh: groups: 2 (over x), tile: 16 (over z, y, core).
Axes of the slice: x: 2, y: 2, z: 4, core: 2. Of those that a mesh axis runs over, the one named last changes fastest.
Arguments:
- tracer: float32 [32, 6, 8, 128, 128], P(('groups', 'tile')), parts along dimension 0, may hold values from -6 to 6
- courant_east: bfloat16 [32, 6, 8, 128, 128], P(('groups', 'tile')), parts along dimension 0, may hold values from -1.5 to 1.5
- courant_north: bfloat16 [32, 6, 8, 128, 128], P(('groups', 'tile')), parts along dimension 0, may hold values from -1.5 to 1.5
- diffusivity: bfloat16 [32, 6, 8, 128, 128], P(('groups', 'tile')), parts along dimension 0, may hold values from 0.049804688 to 5
- seam_table: int32 [6, 4, 3], replicated, may hold values from 0 to 5, as said below
Outputs:
- updated: float32 [32, 6, 8, 128, 128], P(('groups', 'tile')), parts along dimension 0
The draws below stay inside these ranges and needn't reach their ends.
There are 2 independent parts, one for each index of `groups`. The reference program is written for one: setup_inputs(seed, part) draws one part's arguments, and reference() takes and returns one part's arrays. A program takes and returns all parts, laid end to end along the dimension named above; an argument that names none is the same for every part. Nothing has to cross between parts.
Inputs may be any that keep to these rules, and one draw needn't show every extreme that they name: seam_table[p, e] = (q, f, r) names the edge f of panel q != p that borders edge e of panel p, and r is 1 where their edge indices run in opposite directions, 0 otherwise; the 24 edges form 12 pairs whose entries name each other with the same r, as on the faces of a cube ; edge 3 of panel 0 borders edge 3 of panel 1.
All inputs are finite; a program needn't handle non-finite values.
Results may differ from the reference program's by a relative error of at most 0.0003.
Values sent between devices are 32-bit elements; how exact they have to be, the bound alone decides.
No kernel may reach another device: no remote copies, remote signals or barrier semaphores. Data moves between devices by JAX's collectives and lax.ppermute only.
A program may use at most 128 MiB of HBM per device.

```python
import math
import jax
import jax.numpy as jnp
from jax import lax

CT = 128
LEVELS = 8
PANELS = 6
DEPTH = 2
SIDE = 4
N_TILE = 16


def turn_axes(first_old, second_old, quarter):
    first_axis = jnp.where(quarter == 0, first_old, jnp.where(quarter == 1, second_old, jnp.where(quarter == 2, -first_old, -second_old)))
    second_axis = jnp.where(quarter == 0, second_old, jnp.where(quarter == 1, -first_old, jnp.where(quarter == 2, -second_old, first_old)))
    return (first_axis, second_axis)


def draw_seam_table(key, part):
    normals = jnp.array([[1, 0, 0], [0, 1, 0], [0, 0, 1], [-1, 0, 0], [0, -1, 0], [0, 0, -1]], jnp.int32)
    firsts = jnp.array([[0, 1, 0], [0, 0, 1], [1, 0, 0], [0, 0, 1], [1, 0, 0], [0, 1, 0]], jnp.int32)
    seconds = jnp.array([[0, 0, 1], [1, 0, 0], [0, 1, 0], [0, 1, 0], [0, 0, 1], [1, 0, 0]], jnp.int32)
    split_keys = jax.random.split(jax.random.fold_in(key, 11), 3)
    head_label = jax.random.randint(split_keys[0], (1,), 0, 6)
    quarter = jax.random.randint(split_keys[1], (6, 1), 0, 4)
    centre_zero = normals[head_label]
    first_zero, second_zero = turn_axes(firsts[head_label], seconds[head_label], quarter[0:1])
    centre_one = -first_zero
    first_one = -centre_zero
    second_one = -second_zero
    remaining = jnp.concatenate([-centre_zero, first_zero, second_zero, -second_zero], axis=0)
    remaining = remaining[jax.random.permutation(split_keys[2], 4)]
    same_face = jnp.all(remaining[:, None, :] == normals[None, :, :], axis=-1).astype(jnp.int32)
    rest_labels = jnp.sum(same_face * jnp.arange(6, dtype=jnp.int32)[None, :], axis=1)
    first_rest, second_rest = turn_axes(firsts[rest_labels], seconds[rest_labels], quarter[2:])
    centre = jnp.concatenate([centre_zero, centre_one, remaining], axis=0)
    first_axis = jnp.concatenate([first_zero, first_one, first_rest], axis=0)
    second_axis = jnp.concatenate([second_zero, second_one, second_rest], axis=0)
    middle = jnp.stack([centre - second_axis, centre + first_axis, centre + second_axis, centre - first_axis], axis=1).reshape(24, 3)
    heading = jnp.stack([first_axis, second_axis, first_axis, second_axis], axis=1).reshape(24, 3)
    panel_of = jnp.arange(24, dtype=jnp.int32) // 4
    matches = jnp.all(middle[:, None, :] == middle[None, :, :], axis=-1) & (panel_of[:, None] != panel_of[None, :])
    partner = jnp.sum(matches.astype(jnp.int32) * jnp.arange(24, dtype=jnp.int32)[None, :], axis=1)
    partner_heading = jnp.sum(matches.astype(jnp.int32)[:, :, None] * heading[None, :, :], axis=1)
    reversal = (jnp.sum(heading * partner_heading, axis=-1) < 0).astype(jnp.int32)
    return jnp.stack([partner // 4, partner % 4, reversal], axis=-1).reshape(6, 4, 3).astype(jnp.int32)


def steps_of(key, extent, pieces, least, top_value):
    factor_of = 1.0
    for position, blocks in pieces:
        heights = jax.random.uniform(jax.random.fold_in(jax.random.fold_in(key, 6), position), (blocks,), jnp.float32, least / len(pieces), top_value / len(pieces))
        factor_of = factor_of * jnp.repeat(jnp.exp(heights), extent[position] // blocks).reshape((-1,) + (1,) * (len(extent) - 1 - position))
    return factor_of


def bell_draw(own_key, shape, width, limit, cuts=(), held_as=jnp.bfloat16):
    result = jax.random.normal(own_key, shape, jnp.float32) * width
    if len(cuts) > 0:
        result = steps_of(own_key, shape, cuts, -0.22, 0.18) * result
    return jnp.clip(result, min=-limit, max=limit).astype(held_as)


def setup_inputs(seed: int = 0, part: int = 0) -> dict:
    arg_keys = jax.random.split(jax.random.key(seed), 6)
    own_keys = jax.random.split(jax.random.fold_in(arg_keys[5], part), 6)
    tracer = bell_draw(own_keys[0], (N_TILE, PANELS, LEVELS, CT, CT), 1.0, 6.0, ((0, 16),), jnp.float32)
    courant_east = bell_draw(own_keys[1], (N_TILE, PANELS, LEVELS, CT, CT), 0.3, 1.5, ((0, 16),))
    courant_north = bell_draw(own_keys[2], (N_TILE, PANELS, LEVELS, CT, CT), 0.3, 1.5, ((0, 16),))
    diffusivity = jnp.clip(jnp.exp(math.log(5.0) - 4.609084 * jax.random.uniform(own_keys[3], (N_TILE, PANELS, LEVELS, CT, CT), jnp.float32) ** steps_of(own_keys[3], (N_TILE, PANELS, LEVELS, CT, CT), ((0, 16),), -0.2, 0.2)), 0.049804688, 5.0).astype(jnp.bfloat16)
    seam_table = draw_seam_table(jax.random.fold_in(arg_keys[5], 71), part)
    return dict(tracer=tracer, courant_east=courant_east, courant_north=courant_north, diffusivity=diffusivity, seam_table=seam_table)


def edge_strips(panels, rows_deep):
    south_rows = jnp.moveaxis(panels[:, :, :, :rows_deep], 3, 1)
    east_rows = jnp.moveaxis(panels[:, :, ::-1, :][:, :, :rows_deep, :], 2, 1)
    north_rows = jnp.moveaxis(panels[:, :, :, ::-1][:, :, :, :rows_deep], 3, 1)
    west_rows = jnp.moveaxis(panels[:, :, :rows_deep, :], 2, 1)
    return jnp.stack([south_rows, east_rows, north_rows, west_rows], axis=1)


def centered(extended, along):
    kept = extended.shape[along] - 4

    def shifted(offset):
        return lax.slice_in_dim(extended, 2 + offset, 2 + offset + kept, axis=along)

    return (8.0 * (shifted(1) - shifted(-1)) - (shifted(2) - shifted(-2))) / 12.0


def advance(panels, ghosts, courant_east, courant_north, diffusivity):
    west_part = jnp.moveaxis(ghosts[:, 3, ::-1], 1, 2)
    east_part = jnp.moveaxis(ghosts[:, 1], 1, 2)
    south_part = jnp.transpose(ghosts[:, 0, ::-1], (0, 2, 3, 1))
    north_part = jnp.transpose(ghosts[:, 2], (0, 2, 3, 1))
    along_first = jnp.concatenate([west_part, panels, east_part], axis=2)
    along_second = jnp.concatenate([south_part, panels, north_part], axis=3)
    forced = panels - (courant_east.astype(jnp.float32) * centered(along_first, 2)
                       + courant_north.astype(jnp.float32) * centered(along_second, 3))
    coupling = diffusivity.astype(jnp.float32)
    ratios = []
    partial_values = []
    for height in range(panels.shape[1]):
        diagonal = 1.0 + coupling[:, height]
        if height > 0:
            below = coupling[:, height - 1]
            pivot_value = diagonal + below - below * ratios[-1]
            current = (forced[:, height] + below * partial_values[-1]) / pivot_value
        else:
            pivot_value = diagonal
            current = forced[:, height] / pivot_value
        ratios.append(coupling[:, height] / pivot_value)
        partial_values.append(current)
    solved = [partial_values[-1]]
    for height in range(panels.shape[1] - 2, -1, -1):
        solved.insert(0, partial_values[height] + ratios[height] * solved[0])
    return jnp.stack(solved, axis=1)


def panel_offset(panel_no):
    return (panel_no % 2) * (SIDE * SIDE // 2 + 1)


def to_panels(tiles):
    aligned = jnp.stack([jnp.roll(tiles[:, panel_no], -panel_offset(panel_no), axis=0)
                         for panel_no in range(PANELS)], axis=1)
    shaped = aligned.reshape(SIDE, SIDE, PANELS, LEVELS, CT, CT)
    shaped = jnp.transpose(shaped, (2, 3, 0, 4, 1, 5))
    return shaped.reshape(PANELS, LEVELS, SIDE * CT, SIDE * CT)


def to_tiles(panels):
    shaped = panels.reshape(PANELS, LEVELS, SIDE, CT, SIDE, CT)
    shaped = jnp.transpose(shaped, (2, 4, 0, 1, 3, 5))
    aligned = shaped.reshape(SIDE * SIDE, PANELS, LEVELS, CT, CT)
    return jnp.stack([jnp.roll(aligned[:, panel_no], panel_offset(panel_no), axis=0)
                      for panel_no in range(PANELS)], axis=1)


def reference(tracer, courant_east, courant_north, diffusivity, seam_table):
    panels = to_panels(tracer)
    strips = edge_strips(panels, DEPTH)
    flat_strips = strips.reshape((PANELS * 4,) + strips.shape[2:])
    source_block = (seam_table[:, :, 0] * 4 + seam_table[:, :, 1]).reshape(-1).astype(jnp.int32)
    reverse_it = (seam_table[:, :, 2] == 1).reshape(-1)
    picked = jnp.take(flat_strips, source_block, axis=0)
    picked = jnp.where(reverse_it[:, None, None, None], picked[..., ::-1], picked)
    ghosts = picked.reshape(strips.shape)
    updated = advance(panels, ghosts, to_panels(courant_east), to_panels(courant_north), to_panels(diffusivity))
    return to_tiles(updated)
```

```python
import math

import jax
import jax.numpy as jnp
from jax import lax
from jax.experimental import pallas as pl
from jax.experimental.pallas import tpu as pltpu
from jax.sharding import PartitionSpec as P

DEPTH = 2


def split3(x):
    hi = x.astype(jnp.bfloat16)
    rest = x - hi.astype(jnp.float32)
    mid = rest.astype(jnp.bfloat16)
    low = (rest - mid.astype(jnp.float32)).astype(jnp.bfloat16)
    return hi, mid, low


def pack_body(tracer_ref, out_ref, *, levels, cells):
    panel = pl.program_id(0)
    lane = lax.broadcasted_iota(jnp.int32, (cells, cells), 1)
    group = lane // (2 * DEPTH)
    packed = jnp.zeros((cells, cells), jnp.float32)
    for k in range(levels):
        turned = pltpu.roll(tracer_ref[0, k], 2 * DEPTH * k + DEPTH, 1)
        packed = jnp.where(group == k, turned, packed)
    rows = packed.T
    for k in range(levels):
        for d in range(DEPTH):
            m = k * DEPTH + d
            south = 2 * DEPTH * k + DEPTH + d
            north = 2 * DEPTH * k + DEPTH - 1 - d
            out_ref[m, pl.ds(panel * 4, 1), :] = rows[south : south + 1]
            out_ref[m, pl.ds(panel * 4 + 1, 1), :] = tracer_ref[0, k, cells - 1 - d : cells - d, :]
            out_ref[m, pl.ds(panel * 4 + 2, 1), :] = rows[north : north + 1]
            out_ref[m, pl.ds(panel * 4 + 3, 1), :] = tracer_ref[0, k, d : d + 1, :]


def pack(panels):
    count, levels, cells, _ = panels.shape
    return pl.pallas_call(
        lambda a, o: pack_body(a, o, levels=levels, cells=cells),
        grid=(count,),
        in_specs=[pl.BlockSpec((1, levels, cells, cells), lambda p: (p, 0, 0, 0))],
        out_specs=pl.BlockSpec((levels * DEPTH, count * 4, cells), lambda p: (0, 0, 0)),
        out_shape=jax.ShapeDtypeStruct((levels * DEPTH, count * 4, cells), jnp.float32),
        name="pack",
    )(panels)


def route_body(index_ref, rows_ref, out_ref):
    total, cells = rows_ref.shape
    source = lax.broadcasted_iota(jnp.int32, (cells, cells), 0)
    target = lax.broadcasted_iota(jnp.int32, (cells, cells), 1)
    flip = (source + target == cells - 1).astype(jnp.float32).astype(jnp.bfloat16)
    parts = split3(rows_ref[...])
    flipped = [
        jnp.dot(part, flip, preferred_element_type=jnp.float32).astype(jnp.bfloat16)
        for part in parts
    ]
    both = jnp.concatenate(
        [jnp.concatenate(parts, axis=1), jnp.concatenate(flipped, axis=1)], axis=0
    )
    numbers = lax.broadcasted_iota(jnp.int32, (2 * total, index_ref.shape[1]), 0)
    width = index_ref.shape[1]
    for c in range(index_ref.shape[0]):
        chosen = (numbers == index_ref[c : c + 1, :]).astype(jnp.float32).astype(jnp.bfloat16)
        got = lax.dot_general(
            chosen, both, (((0,), (0,)), ((), ())), preferred_element_type=jnp.float32
        )
        out_ref[c * width : (c + 1) * width, :] = (
            got[:, :cells] + got[:, cells : 2 * cells]
        ) + got[:, 2 * cells :]


def route(index, rows):
    return pl.pallas_call(
        route_body,
        out_shape=jax.ShapeDtypeStruct(rows.shape, rows.dtype),
        name="route",
    )(index, rows)


def advance_body(
    tracer_ref, east_ref, north_ref, diff_ref, own_ref, ghost_ref, out_ref, ext_ref, fix_ref,
    *, levels, cells, step,
):
    panel = pl.program_id(0)
    rows = levels * DEPTH

    def strip(ref, edge):
        return ref[0:rows, pl.ds(panel * 4 + edge, 1), :].reshape(rows, cells)

    south = strip(ghost_ref, 0) - strip(own_ref, 2)
    north = strip(ghost_ref, 2) - strip(own_ref, 0)
    parts = [part.astype(jnp.float32) for side in (south, north) for part in split3(side)]
    stacked = jnp.concatenate(parts, axis=0)
    depth_of = lax.broadcasted_iota(jnp.int32, (rows, cells), 0) % DEPTH
    level_of = lax.broadcasted_iota(jnp.int32, (rows, cells), 0) // DEPTH
    lane = lax.broadcasted_iota(jnp.int32, (rows, cells), 1)
    from_south = jnp.where(
        depth_of == 0,
        jnp.where(lane == 0, -8.0, jnp.where(lane == 1, 1.0, 0.0)),
        jnp.where(lane == 0, 1.0, 0.0),
    )
    from_north = jnp.where(
        depth_of == 0,
        jnp.where(lane == cells - 1, 8.0, jnp.where(lane == cells - 2, -1.0, 0.0)),
        jnp.where(lane == cells - 1, -1.0, 0.0),
    )
    spread = jnp.concatenate([from_south] * 3 + [from_north] * 3, axis=0)
    levels_stacked = jnp.concatenate([level_of] * 6, axis=0)
    spread_all = jnp.concatenate(
        [jnp.where(levels_stacked == k, spread, 0.0) for k in range(levels)], axis=1
    ).astype(jnp.bfloat16)
    fix_ref[...] = jnp.dot(
        stacked.T.astype(jnp.bfloat16), spread_all, preferred_element_type=jnp.float32
    )

    for k in range(levels):
        ext_ref[k, 8 : 8 + cells, :] = tracer_ref[0, k]
        for d in range(DEPTH):
            m = k * DEPTH + d
            ext_ref[k, 7 - d : 8 - d, :] = ghost_ref[m, pl.ds(panel * 4 + 3, 1), :]
            ext_ref[k, 8 + cells + d : 9 + cells + d, :] = ghost_ref[
                m, pl.ds(panel * 4 + 1, 1), :
            ]

    for start in range(0, cells, step):
        ratios = []
        partial_values = []
        below = None
        for k in range(levels):

            def shifted(offset):
                return ext_ref[k, 8 + start + offset : 8 + start + offset + step, :]

            q = tracer_ref[0, k, start : start + step, :]
            along_first = 8.0 * (shifted(1) - shifted(-1)) - (shifted(2) - shifted(-2))
            along_second = (
                8.0 * (pltpu.roll(q, cells - 1, 1) - pltpu.roll(q, 1, 1))
                - (pltpu.roll(q, cells - 2, 1) - pltpu.roll(q, 2, 1))
            ) + fix_ref[start : start + step, k * cells : (k + 1) * cells]
            east = east_ref[0, k, start : start + step, :].astype(jnp.float32)
            north_c = north_ref[0, k, start : start + step, :].astype(jnp.float32)
            forced = q - (east * along_first + north_c * along_second) * (1.0 / 12.0)
            coupling = diff_ref[0, k, start : start + step, :].astype(jnp.float32)
            pivot = 1.0 + coupling
            if k > 0:
                pivot = pivot + below - below * ratios[-1]
                forced = forced + below * partial_values[-1]
            inverse = 1.0 / pivot
            ratios.append(coupling * inverse)
            partial_values.append(forced * inverse)
            below = coupling
        value = partial_values[-1]
        out_ref[0, levels - 1, start : start + step, :] = value
        for k in range(levels - 2, -1, -1):
            value = partial_values[k] + ratios[k] * value
            out_ref[0, k, start : start + step, :] = value


def advance(panels, east, north, diff, own, ghosts):
    count, levels, cells, _ = panels.shape
    block = pl.BlockSpec((1, levels, cells, cells), lambda p: (p, 0, 0, 0))
    own_whole = pl.BlockSpec(own.shape, lambda p: (0, 0, 0))
    ghost_whole = pl.BlockSpec((levels * DEPTH,) + ghosts.shape[1:], lambda p: (0, 0, 0))
    return pl.pallas_call(
        lambda *refs: advance_body(*refs, levels=levels, cells=cells, step=16),
        grid=(count,),
        in_specs=[block, block, block, block, own_whole, ghost_whole],
        out_specs=block,
        out_shape=jax.ShapeDtypeStruct(panels.shape, panels.dtype),
        scratch_shapes=[
            pltpu.VMEM((levels, cells + 16, cells), jnp.float32),
            pltpu.VMEM((cells, levels * cells), jnp.float32),
        ],
        name="advance",
    )(panels, east, north, diff, own, ghosts)


def row_sources(seam_table, across):
    total = across * across
    device = jnp.arange(total, dtype=jnp.int32)[:, None]
    slot = jnp.arange(24, dtype=jnp.int32)[None, :]
    panel = slot // 4
    edge = slot % 4
    flat = seam_table.reshape(24, 3)
    far_panel = flat[:, 0][None, :]
    far_edge = flat[:, 1][None, :]
    turned = flat[:, 2][None, :] == 1
    shift = total // 2 + 1
    tile = (device - panel % 2 * shift) % total
    row = tile // across
    col = tile % across
    last = across - 1
    on_edge = jnp.where(
        edge == 0, col == 0, jnp.where(edge == 1, row == last, jnp.where(edge == 2, col == last, row == 0))
    )
    along = jnp.where(edge % 2 == 0, row, col)
    spot = jnp.where(turned, last - along, along)
    far_tile = jnp.where(
        far_edge == 0,
        spot * across,
        jnp.where(far_edge == 1, last * across + spot, jnp.where(far_edge == 2, spot * across + last, spot)),
    )
    far_device = (far_tile + far_panel % 2 * shift) % total
    step = jnp.where(edge == 0, -1, jnp.where(edge == 1, across, jnp.where(edge == 2, 1, -across)))
    near_device = (device + step) % total
    source = jnp.where(
        on_edge,
        far_device * 24 + far_panel * 4 + far_edge,
        near_device * 24 + panel * 4 + (edge + 2) % 4,
    )
    return source + jnp.where(on_edge & turned, total * 24, 0)


def shards(tracer, courant_east, courant_north, diffusivity, seam_table):
    panels = tracer[0]
    tile_count = lax.axis_size("tile")
    across = math.isqrt(tile_count)
    cells = panels.shape[-1]
    own = pack(panels)
    rows = own.shape[0]
    assert tile_count >= rows
    send = own
    if tile_count > rows:
        send = jnp.pad(own, ((0, tile_count - rows), (0, 0), (0, 0)))
    held = lax.all_to_all(send, "tile", 0, 0, tiled=True)
    index = row_sources(seam_table, across).reshape(-1, cells)
    routed = route(index, held.reshape(-1, cells))
    ghosts = lax.all_to_all(routed.reshape(held.shape), "tile", 0, 0, tiled=True)
    updated = advance(
        panels, courant_east[0], courant_north[0], diffusivity[0], own, ghosts
    )
    return updated[None]


def solution(mesh):
    placed = P(("groups", "tile"), None, None, None, None)
    return jax.shard_map(
        shards,
        mesh=mesh,
        in_specs=(placed, placed, placed, placed, P()),
        out_specs=placed,
        check_vma=False,
    )
```

```python
import math

import jax
import jax.numpy as jnp
from jax import lax
from jax.experimental import pallas as pl
from jax.experimental.pallas import tpu as pltpu
from jax.sharding import PartitionSpec as P

DEPTH = 2
EARLY = 3


def split3(x):
    hi = x.astype(jnp.bfloat16)
    rest = x - hi.astype(jnp.float32)
    mid = rest.astype(jnp.bfloat16)
    low = (rest - mid.astype(jnp.float32)).astype(jnp.bfloat16)
    return hi, mid, low


def pack_body(tracer_ref, out_ref, *, count, levels, cells):
    lane = lax.broadcasted_iota(jnp.int32, (cells, cells), 1)
    group = lane // (2 * DEPTH)
    for p in range(count):
        packed = jnp.zeros((cells, cells), jnp.float32)
        for k in range(levels):
            turned = pltpu.roll(tracer_ref[p, k], 2 * DEPTH * k + DEPTH, 1)
            packed = jnp.where(group == k, turned, packed)
        rows = packed.T
        for k in range(levels):
            for d in range(DEPTH):
                m = d * levels + k
                south = 2 * DEPTH * k + DEPTH + d
                north = 2 * DEPTH * k + DEPTH - 1 - d
                slot = p * 4
                out_ref[m, slot : slot + 1, :] = rows[south : south + 1]
                out_ref[m, slot + 1 : slot + 2, :] = tracer_ref[p, k, cells - 1 - d : cells - d, :]
                out_ref[m, slot + 2 : slot + 3, :] = rows[north : north + 1]
                out_ref[m, slot + 3 : slot + 4, :] = tracer_ref[p, k, d : d + 1, :]


def pack(panels):
    total, levels, cells, _ = panels.shape
    count = 2
    return pl.pallas_call(
        lambda a, o: pack_body(a, o, count=count, levels=levels, cells=cells),
        grid=(total // count,),
        in_specs=[pl.BlockSpec((count, levels, cells, cells), lambda p: (p, 0, 0, 0))],
        out_specs=pl.BlockSpec((levels * DEPTH, count * 4, cells), lambda p: (0, p, 0)),
        out_shape=jax.ShapeDtypeStruct((levels * DEPTH, total * 4, cells), jnp.float32),
        name="pack",
    )(panels)


def route_body(index_ref, rows_ref, out_ref):
    total, cells = rows_ref.shape
    source = lax.broadcasted_iota(jnp.int32, (cells, cells), 0)
    target = lax.broadcasted_iota(jnp.int32, (cells, cells), 1)
    flip = (source + target == cells - 1).astype(jnp.float32).astype(jnp.bfloat16)
    parts = split3(rows_ref[...])
    flipped = [
        jnp.dot(part, flip, preferred_element_type=jnp.float32).astype(jnp.bfloat16)
        for part in parts
    ]
    both = jnp.concatenate(
        [jnp.concatenate(parts, axis=1), jnp.concatenate(flipped, axis=1)], axis=0
    )
    numbers = lax.broadcasted_iota(jnp.int32, (2 * total, index_ref.shape[1]), 0)
    width = index_ref.shape[1]
    for c in range(index_ref.shape[0]):
        chosen = (numbers == index_ref[c : c + 1, :]).astype(jnp.float32).astype(jnp.bfloat16)
        got = lax.dot_general(
            chosen, both, (((0,), (0,)), ((), ())), preferred_element_type=jnp.float32
        )
        out_ref[c * width : (c + 1) * width, :] = (
            got[:, :cells] + got[:, cells : 2 * cells]
        ) + got[:, 2 * cells :]


def route(index, rows):
    return pl.pallas_call(
        route_body,
        out_shape=jax.ShapeDtypeStruct(rows.shape, rows.dtype),
        name="route",
    )(index, rows)


def edge_column(line, cells):
    return jnp.where(line < DEPTH, line, cells - 2 * DEPTH + line)


def inner_body(
    tracer_ref, east_ref, north_ref, diff_ref, *refs, levels, cells, step
):
    out_ref, lines_ref, ext_ref, select_ref = refs[-4:]
    lines = 4 * DEPTH

    @pl.when(pl.program_id(0) == 0)
    def _():
        row = lax.broadcasted_iota(jnp.int32, (cells, cells), 0)
        lane = lax.broadcasted_iota(jnp.int32, (cells, cells), 1)
        line = lane % lines
        hit = (row == edge_column(line, cells)) & (line < 2 * DEPTH)
        for n in range(2 * levels):
            select_ref[n] = jnp.where(hit & (lane // lines == n), 1.0, 0.0).astype(jnp.bfloat16)

    columns = jnp.zeros((cells, cells), jnp.float32)
    for k in range(levels):
        columns += jnp.dot(north_ref[0, k], select_ref[k], preferred_element_type=jnp.float32)
        columns += jnp.dot(
            diff_ref[0, k], select_ref[levels + k], preferred_element_type=jnp.float32
        )
    columns = columns.T
    for f, field_ref in ((0, east_ref), (1, diff_ref)):
        for k in range(levels):
            base = (f * levels + k) * lines
            lines_ref[0, f, k, 0 : 2 * DEPTH, :] = columns[base : base + 2 * DEPTH]
            first = field_ref[0, k, 0:16, :].astype(jnp.float32)
            last = field_ref[0, k, cells - 16 : cells, :].astype(jnp.float32)
            lines_ref[0, f, k, 2 * DEPTH : 3 * DEPTH, :] = first[0:DEPTH]
            lines_ref[0, f, k, 3 * DEPTH : 4 * DEPTH, :] = last[16 - DEPTH :]

    for k in range(levels):
        ext_ref[k, 8 : 8 + cells, :] = tracer_ref[0, k]
        ext_ref[k, 0:8, :] = tracer_ref[0, k, cells - 8 : cells, :]
        ext_ref[k, 8 + cells : 16 + cells, :] = tracer_ref[0, k, 0:8, :]

    for start in range(0, cells, step):
        ratios = []
        partial_values = []
        below = None
        for k in range(levels):

            def shifted(offset):
                return ext_ref[k, 8 + start + offset : 8 + start + offset + step, :]

            q = tracer_ref[0, k, start : start + step, :]
            along_first = 8.0 * (shifted(1) - shifted(-1)) - (shifted(2) - shifted(-2))
            along_second = 8.0 * (pltpu.roll(q, cells - 1, 1) - pltpu.roll(q, 1, 1)) - (
                pltpu.roll(q, cells - 2, 1) - pltpu.roll(q, 2, 1)
            )
            east = east_ref[0, k, start : start + step, :].astype(jnp.float32)
            north = north_ref[0, k, start : start + step, :].astype(jnp.float32)
            forced = q - (east * along_first + north * along_second) * (1.0 / 12.0)
            coupling = diff_ref[0, k, start : start + step, :].astype(jnp.float32)
            pivot = 1.0 + coupling
            if k > 0:
                pivot = pivot + below - below * ratios[-1]
                forced = forced + below * partial_values[-1]
            inverse = 1.0 / pivot
            ratios.append(coupling * inverse)
            partial_values.append(forced * inverse)
            below = coupling
        value = partial_values[-1]
        out_ref[0, levels - 1, start : start + step, :] = value
        for k in range(levels - 2, -1, -1):
            value = partial_values[k] + ratios[k] * value
            out_ref[0, k, start : start + step, :] = value


def inner(panels, east, north, diff, first, count, earlier=()):
    total, levels, cells, _ = panels.shape
    lines_shape = (total, 2, levels, 4 * DEPTH, cells)
    block = pl.BlockSpec((1, levels, cells, cells), lambda p: (p + first, 0, 0, 0))
    lines_block = pl.BlockSpec((1,) + lines_shape[1:], lambda p: (p + first, 0, 0, 0, 0))
    return pl.pallas_call(
        lambda *refs: inner_body(*refs, levels=levels, cells=cells, step=16),
        grid=(count,),
        in_specs=[block] * 4 + [pl.BlockSpec(memory_space=pl.ANY)] * len(earlier),
        out_specs=(block, lines_block),
        out_shape=(
            jax.ShapeDtypeStruct(panels.shape, panels.dtype),
            jax.ShapeDtypeStruct(lines_shape, jnp.float32),
        ),
        scratch_shapes=[
            pltpu.VMEM((levels, cells + 16, cells), jnp.float32),
            pltpu.VMEM((2 * levels, cells, cells), jnp.bfloat16),
        ],
        input_output_aliases={4 + n: n for n in range(len(earlier))},
        name="inner",
    )(panels, east, north, diff, *earlier)


def edges_body(
    inner_ref, lines_ref, own_ref, ghost_ref, out_ref, source_ref, spread_ref, *, levels, cells
):
    panel = pl.program_id(0)
    lines = 4 * DEPTH
    depth_rows = levels * lines

    @pl.when(panel == 0)
    def _():
        row = lax.broadcasted_iota(jnp.int32, (depth_rows, cells), 0)
        lane = lax.broadcasted_iota(jnp.int32, (depth_rows, cells), 1)
        line = row % lines
        hit = (lane == edge_column(line, cells)) & (line < 2 * DEPTH)
        for k in range(levels):
            mine = jnp.where(hit & (row // lines == k), 1.0, 0.0).astype(jnp.bfloat16)
            for s in range(3):
                spread_ref[
                    s * depth_rows : (s + 1) * depth_rows, k * cells : (k + 1) * cells
                ] = mine

    def strip(ref, edge, d):
        return ref[d * levels : (d + 1) * levels, pl.ds(panel * 4 + edge, 1), :].reshape(
            levels, cells
        )

    for base, low, high in ((0, 0, 2), (2 * DEPTH, 3, 1)):
        low_0 = strip(ghost_ref, low, 0) - strip(own_ref, high, 0)
        low_1 = strip(ghost_ref, low, 1) - strip(own_ref, high, 1)
        high_0 = strip(ghost_ref, high, 0) - strip(own_ref, low, 0)
        high_1 = strip(ghost_ref, high, 1) - strip(own_ref, low, 1)
        source_ref[:, base, :] = low_1 - 8.0 * low_0
        source_ref[:, base + 1, :] = low_0
        source_ref[:, base + 2, :] = -high_0
        source_ref[:, base + 3, :] = 8.0 * high_0 - high_1

    ratios = []
    partial_values = []
    below = None
    for k in range(levels):
        forced = lines_ref[0, 0, k] * source_ref[k] * (-1.0 / 12.0)
        coupling = lines_ref[0, 1, k]
        pivot = 1.0 + coupling
        if k > 0:
            pivot = pivot + below - below * ratios[-1]
            forced = forced + below * partial_values[-1]
        inverse = 1.0 / pivot
        ratios.append(coupling * inverse)
        partial_values.append(forced * inverse)
        below = coupling
    solved = [partial_values[-1]]
    for k in range(levels - 2, -1, -1):
        solved.insert(0, partial_values[k] + ratios[k] * solved[0])

    parts = split3(jnp.concatenate(solved, axis=0))
    stacked = jnp.concatenate([part.astype(jnp.float32) for part in parts], axis=0)
    added = jnp.dot(
        stacked.T.astype(jnp.bfloat16), spread_ref[...], preferred_element_type=jnp.float32
    )
    for k in range(levels):
        value = inner_ref[0, k] + added[:, k * cells : (k + 1) * cells]
        out_ref[0, k] = value
        out_ref[0, k, 0:DEPTH, :] = value[0:DEPTH] + solved[k][2 * DEPTH : 3 * DEPTH]
        out_ref[0, k, cells - DEPTH : cells, :] = (
            value[cells - DEPTH :] + solved[k][3 * DEPTH :]
        )


def edges(inner_values, lines, own, ghosts):
    count, levels, cells, _ = inner_values.shape
    block = pl.BlockSpec((1, levels, cells, cells), lambda p: (p, 0, 0, 0))
    rows = levels * DEPTH
    strips = pl.BlockSpec((rows,) + own.shape[1:], lambda p: (0, 0, 0))
    depth_rows = levels * 4 * DEPTH
    return pl.pallas_call(
        lambda *refs: edges_body(*refs, levels=levels, cells=cells),
        grid=(count,),
        in_specs=[
            block,
            pl.BlockSpec((1,) + lines.shape[1:], lambda p: (p, 0, 0, 0, 0)),
            strips,
            strips,
        ],
        out_specs=block,
        out_shape=jax.ShapeDtypeStruct(inner_values.shape, inner_values.dtype),
        scratch_shapes=[
            pltpu.VMEM((levels, 4 * DEPTH, cells), jnp.float32),
            pltpu.VMEM((3 * depth_rows, levels * cells), jnp.bfloat16),
        ],
        input_output_aliases={0: 0},
        name="edges",
    )(inner_values, lines, own, ghosts)


def row_sources(seam_table, across, cells):
    total = across * across
    flat = seam_table.reshape(24, 3)
    codes = jnp.tile((flat[:, 0] * 4 + flat[:, 1]) * 2 + flat[:, 2], total).reshape(-1, cells)
    number = lax.broadcasted_iota(jnp.int32, codes.shape, 0) * cells + lax.broadcasted_iota(
        jnp.int32, codes.shape, 1
    )
    device = number // 24
    slot = number % 24
    panel = slot // 4
    edge = slot % 4
    far_panel = codes // 8
    far_edge = codes // 2 % 4
    turned = codes % 2 == 1
    shift = total // 2 + 1
    tile = (device - panel % 2 * shift) % total
    row = tile // across
    col = tile % across
    last = across - 1
    on_edge = jnp.where(
        edge == 0, col == 0, jnp.where(edge == 1, row == last, jnp.where(edge == 2, col == last, row == 0))
    )
    along = jnp.where(edge % 2 == 0, row, col)
    spot = jnp.where(turned, last - along, along)
    far_tile = jnp.where(
        far_edge == 0,
        spot * across,
        jnp.where(far_edge == 1, last * across + spot, jnp.where(far_edge == 2, spot * across + last, spot)),
    )
    far_device = (far_tile + far_panel % 2 * shift) % total
    step = jnp.where(edge == 0, -1, jnp.where(edge == 1, across, jnp.where(edge == 2, 1, -across)))
    near_device = (device + step) % total
    source = jnp.where(
        on_edge,
        far_device * 24 + far_panel * 4 + far_edge,
        near_device * 24 + panel * 4 + (edge + 2) % 4,
    )
    return source + jnp.where(on_edge & turned, total * 24, 0)


def shards(tracer, courant_east, courant_north, diffusivity, seam_table):
    panels = tracer[0]
    fields = (panels, courant_east[0], courant_north[0], diffusivity[0])
    tile_count = lax.axis_size("tile")
    across = math.isqrt(tile_count)
    cells = panels.shape[-1]
    own = pack(panels)
    rows = own.shape[0]
    assert tile_count >= rows
    send = own
    if tile_count > rows:
        send = jnp.pad(own, ((0, tile_count - rows), (0, 0), (0, 0)))
    held = lax.all_to_all(send, "tile", 0, 0, tiled=True)
    early = EARLY
    begun = inner(*fields, 0, early)
    index = row_sources(seam_table, across, cells)
    held, index, begun = lax.optimization_barrier((held, index, begun))
    routed = route(index, held.reshape(-1, cells))
    ghosts = lax.all_to_all(routed.reshape(held.shape), "tile", 0, 0, tiled=True)
    whole = inner(*fields, early, panels.shape[0] - early, begun)
    return edges(*whole, own, ghosts)[None]


def solution(mesh):
    placed = P(("groups", "tile"), None, None, None, None)
    return jax.shard_map(
        shards,
        mesh=mesh,
        in_specs=(placed, placed, placed, placed, P()),
        out_specs=placed,
        check_vma=False,
    )
```

```python
import math

import jax
import jax.numpy as jnp
from jax import lax
from jax.experimental import pallas as pl
from jax.experimental.pallas import tpu as pltpu
from jax.sharding import PartitionSpec as P

DEPTH = 2
EARLY = 3


def split3(x):
    hi = x.astype(jnp.bfloat16)
    rest = x - hi.astype(jnp.float32)
    mid = rest.astype(jnp.bfloat16)
    low = (rest - mid.astype(jnp.float32)).astype(jnp.bfloat16)
    return hi, mid, low


def pack_body(tracer_ref, out_ref, *, count, levels, cells):
    lane = lax.broadcasted_iota(jnp.int32, (cells, cells), 1)
    group = lane // (2 * DEPTH)
    for p in range(count):
        packed = jnp.zeros((cells, cells), jnp.float32)
        for k in range(levels):
            turned = pltpu.roll(tracer_ref[p, k], 2 * DEPTH * k + DEPTH, 1)
            packed = jnp.where(group == k, turned, packed)
        rows = packed.T
        for k in range(levels):
            for d in range(DEPTH):
                m = d * levels + k
                south = 2 * DEPTH * k + DEPTH + d
                north = 2 * DEPTH * k + DEPTH - 1 - d
                slot = p * 4
                out_ref[m, slot : slot + 1, :] = rows[south : south + 1]
                out_ref[m, slot + 1 : slot + 2, :] = tracer_ref[p, k, cells - 1 - d : cells - d, :]
                out_ref[m, slot + 2 : slot + 3, :] = rows[north : north + 1]
                out_ref[m, slot + 3 : slot + 4, :] = tracer_ref[p, k, d : d + 1, :]


def pack(panels):
    total, levels, cells, _ = panels.shape
    count = 2
    return pl.pallas_call(
        lambda a, o: pack_body(a, o, count=count, levels=levels, cells=cells),
        grid=(total // count,),
        in_specs=[pl.BlockSpec((count, levels, cells, cells), lambda p: (p, 0, 0, 0))],
        out_specs=pl.BlockSpec((levels * DEPTH, count * 4, cells), lambda p: (0, p, 0)),
        out_shape=jax.ShapeDtypeStruct((levels * DEPTH, total * 4, cells), jnp.float32),
        name="pack",
    )(panels)


def route_body(index_ref, rows_ref, out_ref):
    total, cells = rows_ref.shape
    source = lax.broadcasted_iota(jnp.int32, (cells, cells), 0)
    target = lax.broadcasted_iota(jnp.int32, (cells, cells), 1)
    flip = (source + target == cells - 1).astype(jnp.float32).astype(jnp.bfloat16)
    parts = split3(rows_ref[...])
    flipped = [
        jnp.dot(part, flip, preferred_element_type=jnp.float32).astype(jnp.bfloat16)
        for part in parts
    ]
    both = jnp.concatenate(
        [jnp.concatenate(parts, axis=1), jnp.concatenate(flipped, axis=1)], axis=0
    )
    width = index_ref.shape[1]
    numbers = lax.broadcasted_iota(jnp.int32, (width, 2 * total), 1).astype(jnp.float32)
    wanted = index_ref[...].astype(jnp.float32)
    for c in range(index_ref.shape[0]):
        spread = jnp.broadcast_to(wanted[c : c + 1, :], (width, width)).T
        spread = jnp.concatenate([spread] * (2 * total // width), axis=1)
        chosen = jnp.where(spread == numbers, 1.0, 0.0).astype(jnp.bfloat16)
        got = jnp.dot(chosen, both, preferred_element_type=jnp.float32)
        out_ref[c * width : (c + 1) * width, :] = (
            got[:, :cells] + got[:, cells : 2 * cells]
        ) + got[:, 2 * cells :]


def route(index, rows):
    return pl.pallas_call(
        route_body,
        out_shape=jax.ShapeDtypeStruct(rows.shape, rows.dtype),
        name="route",
    )(index, rows)


def edge_column(line, cells):
    return (cells - DEPTH + line) % cells


def inner_body(
    tracer_ref, east_ref, north_ref, diff_ref, *refs, levels, cells, step
):
    out_ref, lines_ref, ext_ref, select_ref = refs[-4:]
    lines = 4 * DEPTH

    @pl.when(pl.program_id(0) == 0)
    def _():
        row = lax.broadcasted_iota(jnp.int32, (cells, cells), 0)
        lane = lax.broadcasted_iota(jnp.int32, (cells, cells), 1)
        line = lane % lines
        hit = (row == edge_column(line, cells)) & (line < 2 * DEPTH)
        for n in range(2 * levels):
            select_ref[n] = jnp.where(hit & (lane // lines == n), 1.0, 0.0).astype(jnp.bfloat16)

    columns = jnp.zeros((cells, cells), jnp.float32)
    for k in range(levels):
        columns += jnp.dot(north_ref[0, k], select_ref[k], preferred_element_type=jnp.float32)
        columns += jnp.dot(
            diff_ref[0, k], select_ref[levels + k], preferred_element_type=jnp.float32
        )
    columns = columns.T
    for f, field_ref in ((0, east_ref), (1, diff_ref)):
        for k in range(levels):
            base = (f * levels + k) * lines
            lines_ref[0, f, k, 0 : 2 * DEPTH, :] = columns[base : base + 2 * DEPTH]
            first = field_ref[0, k, 0:16, :].astype(jnp.float32)
            last = field_ref[0, k, cells - 16 : cells, :].astype(jnp.float32)
            lines_ref[0, f, k, 2 * DEPTH : 3 * DEPTH, :] = last[16 - DEPTH :]
            lines_ref[0, f, k, 3 * DEPTH : 4 * DEPTH, :] = first[0:DEPTH]

    for k in range(levels):
        ext_ref[k, 8 : 8 + cells, :] = tracer_ref[0, k]
        ext_ref[k, 0:8, :] = tracer_ref[0, k, cells - 8 : cells, :]
        ext_ref[k, 8 + cells : 16 + cells, :] = tracer_ref[0, k, 0:8, :]

    for start in range(0, cells, step):
        ratios = []
        partial_values = []
        below = None
        for k in range(levels):

            def shifted(offset):
                return ext_ref[k, 8 + start + offset : 8 + start + offset + step, :]

            q = tracer_ref[0, k, start : start + step, :]
            along_first = 8.0 * (shifted(1) - shifted(-1)) - (shifted(2) - shifted(-2))
            along_second = 8.0 * (pltpu.roll(q, cells - 1, 1) - pltpu.roll(q, 1, 1)) - (
                pltpu.roll(q, cells - 2, 1) - pltpu.roll(q, 2, 1)
            )
            east = east_ref[0, k, start : start + step, :].astype(jnp.float32)
            north = north_ref[0, k, start : start + step, :].astype(jnp.float32)
            forced = q - (east * along_first + north * along_second) * (1.0 / 12.0)
            coupling = diff_ref[0, k, start : start + step, :].astype(jnp.float32)
            pivot = 1.0 + coupling
            if k > 0:
                pivot = pivot + below - below * ratios[-1]
                forced = forced + below * partial_values[-1]
            inverse = 1.0 / pivot
            ratios.append(coupling * inverse)
            partial_values.append(forced * inverse)
            below = coupling
        value = partial_values[-1]
        out_ref[0, levels - 1, start : start + step, :] = value
        for k in range(levels - 2, -1, -1):
            value = partial_values[k] + ratios[k] * value
            out_ref[0, k, start : start + step, :] = value


def inner(panels, east, north, diff, first, count, earlier=()):
    total, levels, cells, _ = panels.shape
    lines_shape = (total, 2, levels, 4 * DEPTH, cells)
    block = pl.BlockSpec((1, levels, cells, cells), lambda p: (p + first, 0, 0, 0))
    lines_block = pl.BlockSpec((1,) + lines_shape[1:], lambda p: (p + first, 0, 0, 0, 0))
    return pl.pallas_call(
        lambda *refs: inner_body(*refs, levels=levels, cells=cells, step=16),
        grid=(count,),
        in_specs=[block] * 4 + [pl.BlockSpec(memory_space=pl.ANY)] * len(earlier),
        out_specs=(block, lines_block),
        out_shape=(
            jax.ShapeDtypeStruct(panels.shape, panels.dtype),
            jax.ShapeDtypeStruct(lines_shape, jnp.float32),
        ),
        scratch_shapes=[
            pltpu.VMEM((levels, cells + 16, cells), jnp.float32),
            pltpu.VMEM((2 * levels, cells, cells), jnp.bfloat16),
        ],
        input_output_aliases={4 + n: n for n in range(len(earlier))},
        name="inner",
    )(panels, east, north, diff, *earlier)


def edges_body(inner_ref, lines_ref, own_ref, ghost_ref, out_ref, source_ref, *, levels, cells):
    panel = pl.program_id(0)
    lines = 4 * DEPTH

    def strip(ref, edge, d):
        return ref[d * levels : (d + 1) * levels, pl.ds(panel * 4 + edge, 1), :].reshape(
            levels, cells
        )

    for base, low, high in ((0, 0, 2), (2 * DEPTH, 3, 1)):
        low_0 = strip(ghost_ref, low, 0) - strip(own_ref, high, 0)
        low_1 = strip(ghost_ref, low, 1) - strip(own_ref, high, 1)
        high_0 = strip(ghost_ref, high, 0) - strip(own_ref, low, 0)
        high_1 = strip(ghost_ref, high, 1) - strip(own_ref, low, 1)
        source_ref[:, base, :] = -high_0
        source_ref[:, base + 1, :] = 8.0 * high_0 - high_1
        source_ref[:, base + 2, :] = low_1 - 8.0 * low_0
        source_ref[:, base + 3, :] = low_0

    ratios = []
    partial_values = []
    below = None
    for k in range(levels):
        forced = lines_ref[0, 0, k] * source_ref[k] * (-1.0 / 12.0)
        coupling = lines_ref[0, 1, k]
        pivot = 1.0 + coupling
        if k > 0:
            pivot = pivot + below - below * ratios[-1]
            forced = forced + below * partial_values[-1]
        inverse = 1.0 / pivot
        ratios.append(coupling * inverse)
        partial_values.append(forced * inverse)
        below = coupling
    solved = [partial_values[-1]]
    for k in range(levels - 2, -1, -1):
        solved.insert(0, partial_values[k] + ratios[k] * solved[0])

    blank = jnp.zeros((cells - levels * lines, cells), jnp.float32)
    columns = jnp.concatenate(solved + [blank], axis=0).T
    lane = lax.broadcasted_iota(jnp.int32, (cells, cells), 1)
    outer = (lane < DEPTH) | (lane >= cells - DEPTH)
    for k in range(levels):
        moved = pltpu.roll(columns, (cells - DEPTH - k * lines) % cells, 1)
        value = inner_ref[0, k] + jnp.where(outer, moved, 0.0)
        out_ref[0, k] = value
        out_ref[0, k, 0:DEPTH, :] = value[0:DEPTH] + solved[k][3 * DEPTH :]
        out_ref[0, k, cells - DEPTH : cells, :] = (
            value[cells - DEPTH :] + solved[k][2 * DEPTH : 3 * DEPTH]
        )


def edges(inner_values, lines, own, ghosts):
    count, levels, cells, _ = inner_values.shape
    block = pl.BlockSpec((1, levels, cells, cells), lambda p: (p, 0, 0, 0))
    rows = levels * DEPTH
    strips = pl.BlockSpec((rows,) + own.shape[1:], lambda p: (0, 0, 0))
    return pl.pallas_call(
        lambda *refs: edges_body(*refs, levels=levels, cells=cells),
        grid=(count,),
        in_specs=[
            block,
            pl.BlockSpec((1,) + lines.shape[1:], lambda p: (p, 0, 0, 0, 0)),
            strips,
            strips,
        ],
        out_specs=block,
        out_shape=jax.ShapeDtypeStruct(inner_values.shape, inner_values.dtype),
        scratch_shapes=[
            pltpu.VMEM((levels, 4 * DEPTH, cells), jnp.float32),
        ],
        input_output_aliases={0: 0},
        name="edges",
    )(inner_values, lines, own, ghosts)


def row_sources(seam_table, across, cells):
    total = across * across
    flat = seam_table.reshape(24, 3)
    codes = jnp.tile((flat[:, 0] * 4 + flat[:, 1]) * 2 + flat[:, 2], total).reshape(-1, cells)
    number = lax.broadcasted_iota(jnp.int32, codes.shape, 0) * cells + lax.broadcasted_iota(
        jnp.int32, codes.shape, 1
    )
    device = number // 24
    slot = number % 24
    panel = slot // 4
    edge = slot % 4
    far_panel = codes // 8
    far_edge = codes // 2 % 4
    turned = codes % 2 == 1
    shift = total // 2 + 1
    tile = (device - panel % 2 * shift) % total
    row = tile // across
    col = tile % across
    last = across - 1
    on_edge = jnp.where(
        edge == 0, col == 0, jnp.where(edge == 1, row == last, jnp.where(edge == 2, col == last, row == 0))
    )
    along = jnp.where(edge % 2 == 0, row, col)
    spot = jnp.where(turned, last - along, along)
    far_tile = jnp.where(
        far_edge == 0,
        spot * across,
        jnp.where(far_edge == 1, last * across + spot, jnp.where(far_edge == 2, spot * across + last, spot)),
    )
    far_device = (far_tile + far_panel % 2 * shift) % total
    step = jnp.where(edge == 0, -1, jnp.where(edge == 1, across, jnp.where(edge == 2, 1, -across)))
    near_device = (device + step) % total
    source = jnp.where(
        on_edge,
        far_device * 24 + far_panel * 4 + far_edge,
        near_device * 24 + panel * 4 + (edge + 2) % 4,
    )
    return source + jnp.where(on_edge & turned, total * 24, 0)


def shards(tracer, courant_east, courant_north, diffusivity, seam_table):
    panels = tracer[0]
    fields = (panels, courant_east[0], courant_north[0], diffusivity[0])
    tile_count = lax.axis_size("tile")
    across = math.isqrt(tile_count)
    cells = panels.shape[-1]
    own = pack(panels)
    rows = own.shape[0]
    assert tile_count >= rows
    send = own
    if tile_count > rows:
        send = jnp.pad(own, ((0, tile_count - rows), (0, 0), (0, 0)))
    held = lax.all_to_all(send, "tile", 0, 0, tiled=True)
    early = EARLY
    begun = inner(*fields, 0, early)
    index = row_sources(seam_table, across, cells)
    held, index, begun = lax.optimization_barrier((held, index, begun))
    routed = route(index, held.reshape(-1, cells))
    ghosts = lax.all_to_all(routed.reshape(held.shape), "tile", 0, 0, tiled=True)
    whole = inner(*fields, early, panels.shape[0] - early, begun)
    return edges(*whole, own, ghosts)[None]


def solution(mesh):
    placed = P(("groups", "tile"), None, None, None, None)
    return jax.shard_map(
        shards,
        mesh=mesh,
        in_specs=(placed, placed, placed, placed, P()),
        out_specs=placed,
        check_vma=False,
    )
```

```python
import math

import jax
import jax.numpy as jnp
from jax import lax
from jax.experimental import pallas as pl
from jax.experimental.pallas import tpu as pltpu
from jax.sharding import PartitionSpec as P

DEPTH = 2
EARLY = 3
PIECES = 4


def split3(x):
    hi = x.astype(jnp.bfloat16)
    rest = x - hi.astype(jnp.float32)
    mid = rest.astype(jnp.bfloat16)
    low = (rest - mid.astype(jnp.float32)).astype(jnp.bfloat16)
    return hi, mid, low


def level_parts(count, levels, cells):
    shape = (count, levels // PIECES, cells, cells)
    return [pl.BlockSpec(shape, lambda p, n=n: (p, n, 0, 0)) for n in range(PIECES)]


def pack_body(*refs, count, levels, cells):
    out_ref = refs[-1]
    part = levels // (len(refs) - 1)
    lane = lax.broadcasted_iota(jnp.int32, (cells, cells), 1)
    group = lane // (2 * DEPTH)
    for p in range(count):
        packed = jnp.zeros((cells, cells), jnp.float32)
        for k in range(levels):
            turned = pltpu.roll(refs[k // part][p, k % part], 2 * DEPTH * k + DEPTH, 1)
            packed = jnp.where(group == k, turned, packed)
        rows = packed.T
        for k in range(levels):
            for d in range(DEPTH):
                m = d * levels + k
                south = 2 * DEPTH * k + DEPTH + d
                north = 2 * DEPTH * k + DEPTH - 1 - d
                slot = p * 4
                out_ref[m, slot : slot + 1, :] = rows[south : south + 1]
                out_ref[m, slot + 1 : slot + 2, :] = refs[k // part][
                    p, k % part, cells - 1 - d : cells - d, :
                ]
                out_ref[m, slot + 2 : slot + 3, :] = rows[north : north + 1]
                out_ref[m, slot + 3 : slot + 4, :] = refs[k // part][p, k % part, d : d + 1, :]


def pack(panels):
    total, levels, cells, _ = panels.shape
    count = 2
    return pl.pallas_call(
        lambda *refs: pack_body(*refs, count=count, levels=levels, cells=cells),
        grid=(total // count,),
        in_specs=level_parts(count, levels, cells),
        out_specs=pl.BlockSpec((levels * DEPTH, count * 4, cells), lambda p: (0, p, 0)),
        out_shape=jax.ShapeDtypeStruct((levels * DEPTH, total * 4, cells), jnp.float32),
        name="pack",
    )(*[panels] * PIECES)


def route_body(index_ref, rows_ref, out_ref):
    total, cells = rows_ref.shape
    source = lax.broadcasted_iota(jnp.int32, (cells, cells), 0)
    target = lax.broadcasted_iota(jnp.int32, (cells, cells), 1)
    flip = (source + target == cells - 1).astype(jnp.float32).astype(jnp.bfloat16)
    parts = split3(rows_ref[...])
    flipped = [
        jnp.dot(part, flip, preferred_element_type=jnp.float32).astype(jnp.bfloat16)
        for part in parts
    ]
    both = jnp.concatenate(
        [jnp.concatenate(parts, axis=1), jnp.concatenate(flipped, axis=1)], axis=0
    )
    width = index_ref.shape[1]
    numbers = lax.broadcasted_iota(jnp.int32, (width, 2 * total), 1).astype(jnp.float32)
    wanted = index_ref[...].astype(jnp.float32)
    for c in range(index_ref.shape[0]):
        spread = jnp.broadcast_to(wanted[c : c + 1, :], (width, width)).T
        spread = jnp.concatenate([spread] * (2 * total // width), axis=1)
        chosen = jnp.where(spread == numbers, 1.0, 0.0).astype(jnp.bfloat16)
        got = jnp.dot(chosen, both, preferred_element_type=jnp.float32)
        out_ref[c * width : (c + 1) * width, :] = (
            got[:, :cells] + got[:, cells : 2 * cells]
        ) + got[:, 2 * cells :]


def route(index, rows):
    return pl.pallas_call(
        route_body,
        out_shape=jax.ShapeDtypeStruct(rows.shape, rows.dtype),
        name="route",
    )(index, rows)


def edge_column(line, cells):
    return (cells - DEPTH + line) % cells


def inner_body(
    tracer_ref, east_ref, north_ref, diff_ref, *refs, levels, cells, step
):
    out_ref, lines_ref, ext_ref, select_ref = refs[-4:]
    lines = 4 * DEPTH

    @pl.when(pl.program_id(0) == 0)
    def _():
        row = lax.broadcasted_iota(jnp.int32, (cells, cells), 0)
        lane = lax.broadcasted_iota(jnp.int32, (cells, cells), 1)
        line = lane % lines
        hit = (row == edge_column(line, cells)) & (line < 2 * DEPTH)
        for n in range(2 * levels):
            select_ref[n] = jnp.where(hit & (lane // lines == n), 1.0, 0.0).astype(jnp.bfloat16)

    columns = jnp.zeros((cells, cells), jnp.float32)
    for k in range(levels):
        columns += jnp.dot(north_ref[0, k], select_ref[k], preferred_element_type=jnp.float32)
        columns += jnp.dot(
            diff_ref[0, k], select_ref[levels + k], preferred_element_type=jnp.float32
        )
    columns = columns.T
    for f, field_ref in ((0, east_ref), (1, diff_ref)):
        for k in range(levels):
            base = (f * levels + k) * lines
            lines_ref[0, f, k, 0 : 2 * DEPTH, :] = columns[base : base + 2 * DEPTH]
            first = field_ref[0, k, 0:16, :].astype(jnp.float32)
            last = field_ref[0, k, cells - 16 : cells, :].astype(jnp.float32)
            lines_ref[0, f, k, 2 * DEPTH : 3 * DEPTH, :] = last[16 - DEPTH :]
            lines_ref[0, f, k, 3 * DEPTH : 4 * DEPTH, :] = first[0:DEPTH]

    for k in range(levels):
        ext_ref[k, 8 : 8 + cells, :] = tracer_ref[0, k]
        ext_ref[k, 0:8, :] = tracer_ref[0, k, cells - 8 : cells, :]
        ext_ref[k, 8 + cells : 16 + cells, :] = tracer_ref[0, k, 0:8, :]

    for start in range(0, cells, step):
        ratios = []
        partial_values = []
        below = None
        for k in range(levels):

            def shifted(offset):
                return ext_ref[k, 8 + start + offset : 8 + start + offset + step, :]

            q = tracer_ref[0, k, start : start + step, :]
            along_first = 8.0 * (shifted(1) - shifted(-1)) - (shifted(2) - shifted(-2))
            along_second = 8.0 * (pltpu.roll(q, cells - 1, 1) - pltpu.roll(q, 1, 1)) - (
                pltpu.roll(q, cells - 2, 1) - pltpu.roll(q, 2, 1)
            )
            east = east_ref[0, k, start : start + step, :].astype(jnp.float32)
            north = north_ref[0, k, start : start + step, :].astype(jnp.float32)
            forced = q - (east * along_first + north * along_second) * (1.0 / 12.0)
            coupling = diff_ref[0, k, start : start + step, :].astype(jnp.float32)
            pivot = 1.0 + coupling
            if k > 0:
                pivot = pivot + below - below * ratios[-1]
                forced = forced + below * partial_values[-1]
            inverse = 1.0 / pivot
            ratios.append(coupling * inverse)
            partial_values.append(forced * inverse)
            below = coupling
        value = partial_values[-1]
        out_ref[0, levels - 1, start : start + step, :] = value
        for k in range(levels - 2, -1, -1):
            value = partial_values[k] + ratios[k] * value
            out_ref[0, k, start : start + step, :] = value


def inner(panels, east, north, diff, first, count, earlier=()):
    total, levels, cells, _ = panels.shape
    lines_shape = (total, 2, levels, 4 * DEPTH, cells)
    block = pl.BlockSpec((1, levels, cells, cells), lambda p: (p + first, 0, 0, 0))
    lines_block = pl.BlockSpec((1,) + lines_shape[1:], lambda p: (p + first, 0, 0, 0, 0))
    return pl.pallas_call(
        lambda *refs: inner_body(*refs, levels=levels, cells=cells, step=16),
        grid=(count,),
        in_specs=[block] * 4 + [pl.BlockSpec(memory_space=pl.ANY)] * len(earlier),
        out_specs=(block, lines_block),
        out_shape=(
            jax.ShapeDtypeStruct(panels.shape, panels.dtype),
            jax.ShapeDtypeStruct(lines_shape, jnp.float32),
        ),
        scratch_shapes=[
            pltpu.VMEM((levels, cells + 16, cells), jnp.float32),
            pltpu.VMEM((2 * levels, cells, cells), jnp.bfloat16),
        ],
        input_output_aliases={4 + n: n for n in range(len(earlier))},
        name="inner",
    )(panels, east, north, diff, *earlier)


def edges_body(*refs, levels, cells):
    lines_ref, own_ref, ghost_ref, out_ref, source_ref = refs[-5:]
    part = levels // (len(refs) - 5)
    panel = pl.program_id(0)
    lines = 4 * DEPTH

    def strip(ref, edge, d):
        return ref[d * levels : (d + 1) * levels, pl.ds(panel * 4 + edge, 1), :].reshape(
            levels, cells
        )

    for base, low, high in ((0, 0, 2), (2 * DEPTH, 3, 1)):
        low_0 = strip(ghost_ref, low, 0) - strip(own_ref, high, 0)
        low_1 = strip(ghost_ref, low, 1) - strip(own_ref, high, 1)
        high_0 = strip(ghost_ref, high, 0) - strip(own_ref, low, 0)
        high_1 = strip(ghost_ref, high, 1) - strip(own_ref, low, 1)
        source_ref[:, base, :] = -high_0
        source_ref[:, base + 1, :] = 8.0 * high_0 - high_1
        source_ref[:, base + 2, :] = low_1 - 8.0 * low_0
        source_ref[:, base + 3, :] = low_0

    ratios = []
    partial_values = []
    below = None
    for k in range(levels):
        forced = lines_ref[0, 0, k] * source_ref[k] * (-1.0 / 12.0)
        coupling = lines_ref[0, 1, k]
        pivot = 1.0 + coupling
        if k > 0:
            pivot = pivot + below - below * ratios[-1]
            forced = forced + below * partial_values[-1]
        inverse = 1.0 / pivot
        ratios.append(coupling * inverse)
        partial_values.append(forced * inverse)
        below = coupling
    solved = [partial_values[-1]]
    for k in range(levels - 2, -1, -1):
        solved.insert(0, partial_values[k] + ratios[k] * solved[0])

    blank = jnp.zeros((cells - levels * lines, cells), jnp.float32)
    columns = jnp.concatenate(solved + [blank], axis=0).T
    lane = lax.broadcasted_iota(jnp.int32, (cells, cells), 1)
    outer = (lane < DEPTH) | (lane >= cells - DEPTH)
    for k in range(levels):
        moved = pltpu.roll(columns, (cells - DEPTH - k * lines) % cells, 1)
        value = refs[k // part][0, k % part] + jnp.where(outer, moved, 0.0)
        out_ref[0, k] = value
        out_ref[0, k, 0:DEPTH, :] = value[0:DEPTH] + solved[k][3 * DEPTH :]
        out_ref[0, k, cells - DEPTH : cells, :] = (
            value[cells - DEPTH :] + solved[k][2 * DEPTH : 3 * DEPTH]
        )


def edges(inner_values, lines, own, ghosts):
    count, levels, cells, _ = inner_values.shape
    block = pl.BlockSpec((1, levels, cells, cells), lambda p: (p, 0, 0, 0))
    rows = levels * DEPTH
    strips = pl.BlockSpec((rows,) + own.shape[1:], lambda p: (0, 0, 0))
    return pl.pallas_call(
        lambda *refs: edges_body(*refs, levels=levels, cells=cells),
        grid=(count,),
        in_specs=level_parts(1, levels, cells)
        + [
            pl.BlockSpec((1,) + lines.shape[1:], lambda p: (p, 0, 0, 0, 0)),
            strips,
            strips,
        ],
        out_specs=block,
        out_shape=jax.ShapeDtypeStruct(inner_values.shape, inner_values.dtype),
        scratch_shapes=[
            pltpu.VMEM((levels, 4 * DEPTH, cells), jnp.float32),
        ],
        name="edges",
    )(*[inner_values] * PIECES, lines, own, ghosts)


def row_sources(seam_table, across, cells):
    total = across * across
    flat = seam_table.reshape(24, 3)
    codes = jnp.tile((flat[:, 0] * 4 + flat[:, 1]) * 2 + flat[:, 2], total).reshape(-1, cells)
    number = lax.broadcasted_iota(jnp.int32, codes.shape, 0) * cells + lax.broadcasted_iota(
        jnp.int32, codes.shape, 1
    )
    device = number // 24
    slot = number % 24
    panel = slot // 4
    edge = slot % 4
    far_panel = codes // 8
    far_edge = codes // 2 % 4
    turned = codes % 2 == 1
    shift = total // 2 + 1
    tile = (device - panel % 2 * shift) % total
    row = tile // across
    col = tile % across
    last = across - 1
    on_edge = jnp.where(
        edge == 0, col == 0, jnp.where(edge == 1, row == last, jnp.where(edge == 2, col == last, row == 0))
    )
    along = jnp.where(edge % 2 == 0, row, col)
    spot = jnp.where(turned, last - along, along)
    far_tile = jnp.where(
        far_edge == 0,
        spot * across,
        jnp.where(far_edge == 1, last * across + spot, jnp.where(far_edge == 2, spot * across + last, spot)),
    )
    far_device = (far_tile + far_panel % 2 * shift) % total
    step = jnp.where(edge == 0, -1, jnp.where(edge == 1, across, jnp.where(edge == 2, 1, -across)))
    near_device = (device + step) % total
    source = jnp.where(
        on_edge,
        far_device * 24 + far_panel * 4 + far_edge,
        near_device * 24 + panel * 4 + (edge + 2) % 4,
    )
    return source + jnp.where(on_edge & turned, total * 24, 0)


def shards(tracer, courant_east, courant_north, diffusivity, seam_table):
    panels = tracer[0]
    fields = (panels, courant_east[0], courant_north[0], diffusivity[0])
    tile_count = lax.axis_size("tile")
    across = math.isqrt(tile_count)
    cells = panels.shape[-1]
    own = pack(panels)
    rows = own.shape[0]
    assert tile_count >= rows
    send = own
    if tile_count > rows:
        send = jnp.pad(own, ((0, tile_count - rows), (0, 0), (0, 0)))
    held = lax.all_to_all(send, "tile", 0, 0, tiled=True)
    early = EARLY
    begun = inner(*fields, 0, early)
    index = row_sources(seam_table, across, cells)
    held, index, begun = lax.optimization_barrier((held, index, begun))
    routed = route(index, held.reshape(-1, cells))
    ghosts = lax.all_to_all(routed.reshape(held.shape), "tile", 0, 0, tiled=True)
    whole = inner(*fields, early, panels.shape[0] - early, begun)
    return edges(*whole, own, ghosts)[None]


def solution(mesh):
    placed = P(("groups", "tile"), None, None, None, None)
    return jax.shard_map(
        shards,
        mesh=mesh,
        in_specs=(placed, placed, placed, placed, P()),
        out_specs=placed,
        check_vma=False,
    )
```
